32 devices in a mesh: sweep: 2 (over y), expert: 4 (over z), dp: 4 (over x, core).
Axes of the slice: x: 2, y: 2, z: 4, core: 2. Of those that a mesh axis runs over, the one named last changes fastest.
Arguments:
- tokens: bfloat16 [4096, 1536], P(('sweep', 'expert', 'dp')), parts along dimension 0, may hold values from -6 to 6
- expert_ids: int32 [4096, 8], P(('sweep', 'expert', 'dp')), parts along dimension 0, may hold values from 0 to 63, all different within a row; in each aligned block of 128 rows (0 to 127, 128 to 255, ...) at most 20 rows name the same one
- gate_weights: float32 [4096, 8], P(('sweep', 'expert', 'dp')), parts along dimension 0, may hold values from 0.1 to 0.6
- expert_in: bfloat16 [128, 1536, 768], P(('sweep', 'expert'), 'dp'), parts along dimension 0, may hold values from -0.15625 to 0.15625
- expert_out: bfloat16 [128, 768, 1536], P(('sweep', 'expert'), None, 'dp'), parts along dimension 0, may hold values from -0.21875 to 0.21875
- shared_in: bfloat16 [3072, 768], P(('sweep', 'dp')), parts along dimension 0, may hold values from -0.15625 to 0.15625
- shared_out: bfloat16 [1536, 1536], P('sweep', 'dp'), parts along dimension 0, may hold values from -0.21875 to 0.21875
Outputs:
- block_out: bfloat16 [4096, 1536], P(('sweep', 'expert', 'dp')), parts along dimension 0
The draws below stay inside these ranges and needn't reach their ends.
There are 2 independent parts, one for each index of `sweep`. The reference program is written for one: setup_inputs(seed, part) draws one part's arguments, and reference() takes and returns one part's arrays. A program takes and returns all parts, laid end to end along the dimension named above; each array names one. Nothing has to cross between parts.
Inputs may be any that keep to these rules, and one draw needn't show every extreme that they name: `expert_ids`: each token names 8 different experts. In each aligned block of 128 tokens (the tokens of one device) no expert is named by more than 20 tokens; some blocks have an expert named by exactly 20.
All inputs are finite; a program needn't handle non-finite values.
Results may differ from the reference program's by a relative error of at most 0.0051.
Values may be sent and summed in bfloat16 or wider, within the bound.
A program may use at most 192 MiB of HBM per device.

```python
import math
import jax
import jax.numpy as jnp
import numpy as np
from jax import lax

D = 1536
FF = 768
EXPERTS = 64
TOPK = 8
TOK_DEV = 128
CAP = 20
TOKENS = 2048


def levels(rng, shape, split, least, top_value):
    def one(position, parts):
        heights = jax.random.uniform(jax.random.fold_in(jax.random.fold_in(rng, 6), position), (parts,), jnp.float32, least / len(split), top_value / len(split))
        return jnp.repeat(jnp.exp(heights), shape[position] // parts).reshape((-1,) + (1,) * (len(shape) - position - 1))

    loudness = one(*split[0])
    for cut in split[1:]:
        loudness = loudness * one(*cut)
    return loudness


def assign_block(key, own, number, rows, amount, top, reach, slope):
    sequence = jax.random.permutation(key, amount)
    heavy_load, usual = load_shares(amount, rows * top, reach, slope, True), load_shares(amount, rows * top, reach, slope, False)
    places = jnp.arange(amount)

    def named(lengths, rotation):
        used = int((lengths > 0).sum())
        fixed = max(1, used // 4)
        moved = fixed + (places - fixed + rotation * (used - fixed)) % max(1, amount - fixed)
        return jnp.zeros((amount,), jnp.int32).at[sequence[jnp.where(places < fixed, places, moved)]].set(jnp.asarray(lengths, jnp.int32))

    lengths = jnp.where(number % 4 == 0, named(heavy_load, number // 4), named(usual, number - number // 4 - 1))
    mixed = jax.random.permutation(jax.random.fold_in(own, 3), amount)
    donor, taker = mixed[0:amount // 2 * 2:2], mixed[1:amount // 2 * 2:2]
    margin = jnp.minimum(lengths[donor] - 1, reach - lengths[taker]) // 2
    margin = jnp.where((donor == sequence[0]) | (taker == sequence[0]) | (lengths[taker] == 0), 0, jnp.maximum(margin, 0))
    moved = jax.random.randint(jax.random.fold_in(own, 4), (amount // 2,), 0, 1 << 20) % (margin + 1)
    lengths = lengths.at[donor].add(-moved).at[taker].add(moved)
    labels = jnp.searchsorted(jnp.cumsum(lengths), jnp.arange(rows * top), side="right").astype(jnp.int32)
    listing = labels.reshape(top, rows).T
    listing = listing[jax.random.permutation(jax.random.fold_in(own, 1), rows)]
    rotation = jax.random.randint(jax.random.fold_in(own, 2), (rows, 1), 0, top)
    return jnp.take_along_axis(listing, (jnp.arange(top)[None, :] + rotation) % top, axis=1)


def load_shares(amount, total, reach, lean, full):
    loads = [(1 << 20) // math.isqrt(grade ** lean) + 1 for grade in range(1, amount + 1)]
    largest = reach if full else min(reach, max(-(-total // amount), total * loads[0] // sum(loads)))
    least = 1 if total - largest >= amount - 1 else 0
    given, spare = [largest] + [least] * (amount - 1), total - largest - least * (amount - 1)
    while spare > 0:
        movable = [i for i in range(1, amount) if given[i] < largest] or [i for i in range(1, amount) if given[i] < reach]
        mass, budget = sum([loads[i] for i in movable]), spare
        for i in movable:
            extra = min(reach - given[i], max(1, budget * loads[i] // mass), spare)
            given[i] = given[i] + extra
            spare = spare - extra
    return np.array(given)


def scatter_about(own_key, dims, scale, limit, cuts=(), kind=jnp.bfloat16):
    level = levels(own_key, dims, cuts, -0.22, 0.18) if cuts else 1.0
    values = jax.random.normal(own_key, dims, jnp.float32) * scale * level
    return jnp.minimum(jnp.maximum(values, -limit), limit).astype(kind)


def setup_inputs(seed: int = 0, part: int = 0) -> dict:
    seeds = jax.random.split(jax.random.key(seed), 8)
    part_splits = jax.random.split(jax.random.fold_in(seeds[7], part), 8)
    tokens = scatter_about(part_splits[0], (TOKENS, D), 1.0, 6.0, ((0, 16),))
    expert_ids_keys = jax.random.split(jax.random.fold_in(part_splits[1], 1), TOKENS // TOK_DEV)
    expert_ids_turns = jax.random.permutation(jax.random.fold_in(part_splits[1], 3), TOKENS // TOK_DEV)
    expert_ids = jax.vmap(lambda own, number: assign_block(jax.random.fold_in(part_splits[1], 2), own, number, TOK_DEV, EXPERTS, TOPK, CAP, 2))(expert_ids_keys, expert_ids_turns).reshape((TOKENS, TOPK))
    gate_weights = jnp.clip(0.1 + 0.5 * jax.random.uniform(part_splits[2], (TOKENS, TOPK), jnp.float32) ** levels(part_splits[2], (TOKENS, TOPK), ((0, 16),), -0.2, 0.2), 0.1, 0.6)
    expert_in = scatter_about(part_splits[3], (EXPERTS, D, FF), D ** -0.5, 0.15625, ((0, 4), (1, 4)))
    expert_out = scatter_about(part_splits[4], (EXPERTS, FF, D), FF ** -0.5, 0.21875, ((0, 4), (2, 4)))
    shared_in = scatter_about(part_splits[5], (D, FF), D ** -0.5, 0.15625, ((0, 4),))
    shared_out = scatter_about(part_splits[6], (FF, D), FF ** -0.5, 0.21875, ((1, 4),))
    return dict(tokens=tokens, expert_ids=expert_ids, gate_weights=gate_weights, expert_in=expert_in, expert_out=expert_out, shared_in=shared_in, shared_out=shared_out)


def layer_norm(tokens):
    values = tokens.astype(jnp.float32)
    center = values - lax.optimization_barrier(jnp.mean(values, axis=-1, keepdims=True))
    spread = lax.optimization_barrier(jnp.mean(center * center, axis=-1, keepdims=True))
    return (center * lax.rsqrt(spread + 1e-06)).astype(jnp.bfloat16)

def reference(tokens, expert_ids, gate_weights, expert_in, expert_out, shared_in, shared_out):
    normed = layer_norm(tokens)
    token_count = tokens.shape[0]
    model_width = tokens.shape[1]
    expert_count = expert_in.shape[0]
    place_count = token_count // TOK_DEV * CAP
    expert_iota = jnp.arange(expert_count, dtype=jnp.int32)
    matches = (expert_ids[:, :, None] == expert_iota[None, None, :]).astype(jnp.int32)
    per_token = lax.optimization_barrier(jnp.sum(matches, axis=1, dtype=jnp.int32))
    earlier = jnp.cumsum(per_token, axis=0, dtype=jnp.int32) - per_token
    slot_of = jnp.take_along_axis(earlier, expert_ids, axis=1).astype(jnp.int32)
    anchors = jnp.broadcast_to(jnp.arange(token_count, dtype=jnp.int32)[:, None], expert_ids.shape)
    slot_table = jnp.full((expert_count, place_count), token_count, jnp.int32)
    slot_table = slot_table.at[expert_ids, slot_of].set(anchors)
    gate_table = jnp.zeros((expert_count, place_count), jnp.float32)
    gate_table = gate_table.at[expert_ids, slot_of].set(gate_weights.astype(jnp.float32))
    padded = jnp.concatenate([normed, jnp.zeros((1, model_width), jnp.bfloat16)], axis=0)

    def expert_step(summed, inputs):
        row_index, gate_rows, weight_in, weight_out = inputs
        gathered = padded[row_index]
        hidden = jax.nn.gelu(jnp.dot(gathered, weight_in, preferred_element_type=jnp.float32)).astype(jnp.bfloat16)
        result = jnp.dot(hidden, weight_out, preferred_element_type=jnp.float32).astype(jnp.bfloat16)
        summed = summed.at[row_index].add(result.astype(jnp.float32) * gate_rows[:, None])
        return (summed, None)
    start_sum = jnp.zeros((token_count + 1, model_width), jnp.float32)
    summed, _ = lax.scan(expert_step, start_sum, (slot_table, gate_table, expert_in, expert_out))
    routed = summed[:token_count]
    shared_hidden = jax.nn.gelu(jnp.dot(normed, shared_in, preferred_element_type=jnp.float32)).astype(jnp.bfloat16)
    shared_result = jnp.dot(shared_hidden, shared_out, preferred_element_type=jnp.float32)
    return (tokens.astype(jnp.float32) + shared_result + routed).astype(jnp.bfloat16)
```

```python
import functools

import jax
import jax.numpy as jnp
from jax import lax
from jax.experimental import pallas as pl
from jax.experimental.pallas import tpu as pltpu
from jax.sharding import PartitionSpec as P

CAP = 20
GROUP = 4


def layer_norm(tokens):
    values = tokens.astype(jnp.float32)
    center = values - jnp.mean(values, axis=-1, keepdims=True)
    spread = jnp.mean(center * center, axis=-1, keepdims=True)
    return (center * lax.rsqrt(spread + 1e-06)).astype(jnp.bfloat16)


def first_kernel(runs, run_tokens, x_ref, key_ref, w_ref, out_ref, rows_ref):
    slots = out_ref.shape[3]
    for j in range(runs):
        span = slice(j * run_tokens, (j + 1) * run_tokens)
        row = lax.broadcasted_iota(jnp.int32, (slots, run_tokens), 0)
        pick = jnp.where(row == key_ref[0, :, span], 1.0, 0.0).astype(jnp.bfloat16)
        rows_ref[j * slots : (j + 1) * slots, :] = jnp.dot(
            pick, x_ref[span, :], preferred_element_type=jnp.float32
        ).astype(jnp.bfloat16)
    pre = jnp.dot(rows_ref[...], w_ref[0], preferred_element_type=jnp.float32)
    for j in range(runs):
        out_ref[j, 0, 0] = pre[j * slots : (j + 1) * slots].astype(jnp.bfloat16)


def first_projection(x, keys, weight, first, count, runs, run_tokens, slots):
    width, hidden = weight.shape[1:]
    chunk = runs * run_tokens
    chunks = x.shape[0] // chunk
    total = count * chunks * runs * slots
    return pl.pallas_call(
        functools.partial(first_kernel, runs, run_tokens),
        grid=(count, chunks),
        in_specs=[
            pl.BlockSpec((chunk, width), lambda e, c: (c, 0)),
            pl.BlockSpec((1, 1, chunk), lambda e, c: (e + first, 0, c)),
            pl.BlockSpec((1, width, hidden), lambda e, c: (e + first, 0, 0)),
        ],
        out_specs=pl.BlockSpec((runs, 1, 1, slots, hidden), lambda e, c: (0, e, c, 0, 0)),
        out_shape=jax.ShapeDtypeStruct((runs, count, chunks, slots, hidden), jnp.bfloat16),
        scratch_shapes=[pltpu.VMEM((runs * slots, width), jnp.bfloat16)],
        cost_estimate=pl.CostEstimate(
            flops=2 * total * width * (hidden + run_tokens),
            bytes_accessed=2 * (count * width * hidden + total * hidden + x.size),
            transcendentals=0,
        ),
    )(x, keys, weight)


def second_kernel(runs, run_tokens, h_ref, key_ref, gate_ref, w_ref, *refs):
    carry_ref, (out_ref, total_ref) = refs[0] if len(refs) == 3 else None, refs[-2:]
    expert = pl.program_id(1)
    slots = h_ref.shape[3]

    @pl.when(expert == 0)
    def _():
        total_ref[...] = jnp.zeros_like(total_ref) if carry_ref is None else carry_ref[...]

    h = jnp.concatenate([h_ref[j, 0, 0] for j in range(runs)], axis=0)
    result = jnp.dot(h, w_ref[0], preferred_element_type=jnp.float32)
    for j in range(runs):
        span = slice(j * run_tokens, (j + 1) * run_tokens)
        row = lax.broadcasted_iota(jnp.int32, (slots, run_tokens), 0)
        match = row == key_ref[0, :, span]
        gate = jnp.sum(jnp.where(match, gate_ref[0, :, span], 0.0), axis=1, keepdims=True)
        scaled = (result[j * slots : (j + 1) * slots] * gate).astype(jnp.bfloat16)
        total_ref[span, :] += lax.dot_general(
            jnp.where(match, 1.0, 0.0).astype(jnp.bfloat16),
            scaled,
            (((0,), (0,)), ((), ())),
            preferred_element_type=jnp.float32,
        )

    @pl.when(expert == pl.num_programs(1) - 1)
    def _():
        out_ref[...] = total_ref[...].astype(out_ref.dtype)


def second_projection(hidden, keys, gates, weight, carry, kind, first, runs, run_tokens):
    _, count, chunks, slots, depth = hidden.shape
    width = weight.shape[2]
    chunk = runs * run_tokens
    total = count * chunks * runs * slots
    carries = [] if carry is None else [carry]
    return pl.pallas_call(
        functools.partial(second_kernel, runs, run_tokens),
        grid=(chunks, count),
        in_specs=[
            pl.BlockSpec((runs, 1, 1, slots, depth), lambda c, e: (0, e, c, 0, 0)),
            pl.BlockSpec((1, 1, chunk), lambda c, e: (e + first, 0, c)),
            pl.BlockSpec((1, 1, chunk), lambda c, e: (e + first, 0, c)),
            pl.BlockSpec((1, depth, width), lambda c, e: (e + first, 0, 0)),
        ]
        + [pl.BlockSpec((chunk, width), lambda c, e: (c, 0)) for _ in carries],
        out_specs=pl.BlockSpec((chunk, width), lambda c, e: (c, 0)),
        out_shape=jax.ShapeDtypeStruct((chunks * chunk, width), kind),
        scratch_shapes=[pltpu.VMEM((chunk, width), jnp.float32)],
        cost_estimate=pl.CostEstimate(
            flops=2 * total * width * (depth + 3 * run_tokens),
            bytes_accessed=2 * (count * depth * width + total * depth) + 4 * chunks * chunk * width,
            transcendentals=0,
        ),
    )(hidden, keys, gates, weight, *carries)


def per_device(tokens, expert_ids, gate_weights, expert_in, expert_out, shared_in, shared_out):
    row_count, model_width = tokens.shape
    pick_count = expert_ids.shape[1]
    local_count = expert_in.shape[0]
    runs = lax.axis_size("dp")
    block_count = runs * lax.axis_size("expert")
    run_tokens = GROUP * row_count
    slots = GROUP * CAP
    halves = 2 if local_count % 2 == 0 else 1

    normed = layer_norm(tokens)
    full_shared_in = lax.all_gather(shared_in, "dp", axis=0, tiled=True)
    full_shared_out = lax.all_gather(shared_out, "dp", axis=1, tiled=True)

    named = jnp.concatenate([expert_ids.astype(jnp.float32), gate_weights], axis=1).T
    named = lax.all_gather(named, ("expert", "dp"), axis=0, tiled=False)
    ids, gates = named[:, :pick_count], named[:, pick_count:]
    columns = lax.all_to_all(normed, "dp", split_axis=1, concat_axis=0, tiled=True)
    x = lax.all_gather(columns, "expert", axis=0, tiled=True)

    owned = lax.axis_index("expert") * local_count + jnp.arange(local_count, dtype=jnp.int32)
    matches = ids[:, :, None, :] == owned.astype(jnp.float32)[:, None]
    chosen = jnp.any(matches, axis=1)
    gate_of = jnp.sum(jnp.where(matches, gates[:, :, None, :], 0.0), axis=1)
    order = jnp.arange(row_count, dtype=jnp.int32)
    before = (order[:, None] < order[None, :]).astype(jnp.bfloat16)
    earlier = jnp.einsum(
        "bej,ji->bei", chosen.astype(jnp.bfloat16), before, preferred_element_type=jnp.float32
    ).astype(jnp.int32)
    base = jnp.arange(block_count, dtype=jnp.int32) % GROUP * CAP
    keys = jnp.where(chosen, earlier + base[:, None, None], -1)

    def by_expert(table):
        return table.transpose(1, 0, 2).reshape(local_count, 1, block_count * row_count)

    keys, gate_of = by_expert(keys), by_expert(gate_of)

    count = local_count // halves
    parts = []
    for half in range(halves):
        pre = first_projection(
            x, keys, expert_in, half * count, count, runs, run_tokens, slots
        )
        parts.append(lax.psum_scatter(pre, "dp", scatter_dimension=0, tiled=True))

    hidden = []
    for pre in parts:
        act = jax.nn.gelu(pre.astype(jnp.float32)).astype(jnp.bfloat16)
        hidden.append(lax.all_gather(act, "dp", axis=0, tiled=True))

    shared_pre = jnp.dot(normed, full_shared_in, preferred_element_type=jnp.float32)
    shared_hidden = jax.nn.gelu(shared_pre).astype(jnp.bfloat16)
    shared_result = jnp.dot(shared_hidden, full_shared_out, preferred_element_type=jnp.float32)

    routed = None
    for half, h in enumerate(hidden):
        kind = jnp.bfloat16 if half == halves - 1 else jnp.float32
        routed = second_projection(
            h, keys, gate_of, expert_out, routed, kind, half * count, runs, run_tokens
        )
    summed = lax.psum_scatter(routed, "expert", scatter_dimension=0, tiled=True)
    own = lax.all_to_all(summed, "dp", split_axis=0, concat_axis=1, tiled=True)
    return (tokens.astype(jnp.float32) + shared_result + own.astype(jnp.float32)).astype(
        jnp.bfloat16
    )


def solution(mesh):
    placed = (
        P(("sweep", "expert", "dp"), None),
        P(("sweep", "expert", "dp"), None),
        P(("sweep", "expert", "dp"), None),
        P(("sweep", "expert"), "dp", None),
        P(("sweep", "expert"), None, "dp"),
        P(("sweep", "dp"), None),
        P("sweep", "dp"),
    )
    return jax.shard_map(
        per_device,
        mesh=mesh,
        in_specs=placed,
        out_specs=P(("sweep", "expert", "dp"), None),
        check_vma=False,
    )
```
